32 devices in a mesh: dp: 4 (over y, z), tp: 8 (over x, core).
Axes of the slice: x: 4, y: 2, z: 2, core: 2. Of those that a mesh axis runs over, the one named last changes fastest.
The devices are a block of a 4x4x8 slice.
Arguments:
- tok_ids: int32 [16, 1536], P('dp'), parts along dimension 0
- pad_mask: int32 [16, 1536], P('dp'), parts along dimension 0
- emb_table: bfloat16 [250880, 2048], P('tp')
- ln_emb_w: bfloat16 [2048], replicated
- ln_emb_b: bfloat16 [2048], replicated
- ln1_w: bfloat16 [2048], replicated
- ln1_b: bfloat16 [2048], replicated
- w_qkv: bfloat16 [2048, 16, 3, 128], P(None, 'tp')
- b_qkv: bfloat16 [16, 3, 128], P('tp')
- w_out: bfloat16 [2048, 2048], P('tp')
- b_out: bfloat16 [2048], replicated
- ln2_w: bfloat16 [2048], replicated
- ln2_b: bfloat16 [2048], replicated
- w_up: bfloat16 [2048, 8192], P(None, 'tp')
- b_up: bfloat16 [8192], P('tp')
- w_down: bfloat16 [8192, 2048], P('tp')
- b_down: bfloat16 [2048], replicated
Outputs:
- output: bfloat16 [16, 1536, 2048], P('dp', 'tp'), parts along dimension 0
There are 4 independent parts. The reference program is written for one: setup_inputs(seed, part) draws one part's arguments, and reference() takes and returns one part's arrays. A program takes and returns all parts, laid end to end along the dimension named above; an argument that names none is the same for every part.
All inputs are finite; a program needn't handle non-finite values.
Results may differ from the reference program's by a relative error of at most 0.0139903.
Values are sent between devices in bfloat16 or wider.
A program may use at most 768 MiB of HBM per device.

```python
import math
import jax
import jax.numpy as jnp
from jax import lax

VOCAB = 250880
D = 2048
HEADS = 16
BATCH = 4
SEQ = 1536
HEAD_DIM = D // HEADS
LN_EPS = 1e-5


def alibi_slopes(n_heads):
    closest = 2 ** int(math.floor(math.log2(n_heads)))
    base_ratio = 2.0 ** (-(2.0 ** -(math.log2(closest) - 3)))
    extra_ratio = 2.0 ** (-(2.0 ** -(math.log2(2 * closest) - 3)))
    first_part = [base_ratio ** step_k for step_k in range(1, closest + 1)]
    second_part = [extra_ratio ** step_k for step_k in range(1, 2 * (n_heads - closest), 2)]
    return first_part + second_part


def layer_norm(values_in, ln_gain, ln_shift):
    values_in = values_in.astype(jnp.float32)
    mean_v = jnp.mean(values_in, axis=-1, keepdims=True)
    centered = values_in - mean_v
    var_v = jnp.mean(centered * centered, axis=-1, keepdims=True)
    scaled = centered * lax.rsqrt(var_v + LN_EPS)
    return (scaled * ln_gain.astype(jnp.float32) + ln_shift.astype(jnp.float32)).astype(jnp.bfloat16)


def bloom_gelu(values_in):
    return values_in * 0.5 * (1.0 + jnp.tanh(0.79788456 * values_in * (1.0 + 0.044715 * values_in * values_in)))


def setup_inputs(seed: int = 0, part: int = 0) -> dict:
    root_key = jax.random.key(seed)
    part_key = jax.random.fold_in(root_key, part)
    id_key, coin_key, pad_key = jax.random.split(part_key, 3)
    raw_ids = jax.random.randint(id_key, (BATCH, SEQ), 0, VOCAB)
    coin_flips = jax.random.randint(coin_key, (BATCH, SEQ), 0, 2)
    tok_ids = jnp.where(coin_flips == 1, raw_ids // 16, raw_ids).astype(jnp.int32)
    tok_ids = tok_ids.at[0, SEQ - 2].set(0).at[0, SEQ - 1].set(VOCAB - 1)
    pad_len = jax.random.randint(pad_key, (BATCH, 1), 0, SEQ // 2 + 1)
    pad_len = pad_len.at[0, 0].set(SEQ // 2)
    pad_mask = (jnp.arange(SEQ)[None, :] >= pad_len).astype(jnp.int32)
    shared = jax.random.split(root_key, 15)
    emb_table = jax.random.normal(shared[0], (VOCAB, D), jnp.float32).astype(jnp.bfloat16)
    ln_emb_w = (1.0 + 0.3 * jax.random.normal(shared[1], (D,), jnp.float32)).astype(jnp.bfloat16)
    ln_emb_b = (0.3 * jax.random.normal(shared[2], (D,), jnp.float32)).astype(jnp.bfloat16)
    ln1_w = (1.0 + 0.3 * jax.random.normal(shared[3], (D,), jnp.float32)).astype(jnp.bfloat16)
    ln1_b = (0.3 * jax.random.normal(shared[4], (D,), jnp.float32)).astype(jnp.bfloat16)
    w_qkv = (jax.random.normal(shared[5], (D, HEADS, 3, HEAD_DIM), jnp.float32) * D ** -0.5).astype(jnp.bfloat16)
    b_qkv = (0.3 * jax.random.normal(shared[6], (HEADS, 3, HEAD_DIM), jnp.float32)).astype(jnp.bfloat16)
    w_out = (jax.random.normal(shared[7], (D, D), jnp.float32) * D ** -0.5).astype(jnp.bfloat16)
    b_out = (0.3 * jax.random.normal(shared[8], (D,), jnp.float32)).astype(jnp.bfloat16)
    ln2_w = (1.0 + 0.3 * jax.random.normal(shared[9], (D,), jnp.float32)).astype(jnp.bfloat16)
    ln2_b = (0.3 * jax.random.normal(shared[10], (D,), jnp.float32)).astype(jnp.bfloat16)
    w_up = (jax.random.normal(shared[11], (D, 4 * D), jnp.float32) * D ** -0.5).astype(jnp.bfloat16)
    b_up = (0.3 * jax.random.normal(shared[12], (4 * D,), jnp.float32)).astype(jnp.bfloat16)
    w_down = (jax.random.normal(shared[13], (4 * D, D), jnp.float32) * (4 * D) ** -0.5).astype(jnp.bfloat16)
    b_down = (0.3 * jax.random.normal(shared[14], (D,), jnp.float32)).astype(jnp.bfloat16)
    return dict(tok_ids=tok_ids, pad_mask=pad_mask, emb_table=emb_table, ln_emb_w=ln_emb_w, ln_emb_b=ln_emb_b, ln1_w=ln1_w, ln1_b=ln1_b, w_qkv=w_qkv, b_qkv=b_qkv, w_out=w_out, b_out=b_out, ln2_w=ln2_w, ln2_b=ln2_b, w_up=w_up, b_up=b_up, w_down=w_down, b_down=b_down)


def reference(tok_ids, pad_mask, emb_table, ln_emb_w, ln_emb_b, ln1_w, ln1_b, w_qkv, b_qkv, w_out, b_out, ln2_w, ln2_b, w_up, b_up, w_down, b_down):
    embedded = jnp.take(emb_table, tok_ids, axis=0)
    resid_in = layer_norm(embedded, ln_emb_w, ln_emb_b).reshape(BATCH * SEQ, D)
    normed = layer_norm(resid_in, ln1_w, ln1_b)
    qkv_flat = jnp.dot(normed, w_qkv.reshape(D, 3 * D), preferred_element_type=jnp.float32) + b_qkv.reshape(3 * D).astype(jnp.float32)
    qkv_all = qkv_flat.astype(jnp.bfloat16).reshape(BATCH, SEQ, HEADS, 3, HEAD_DIM)
    slopes = jnp.array(alibi_slopes(HEADS), jnp.float32)
    positions = jnp.arange(SEQ)
    distance = (positions[None, :] - positions[:, None]).astype(jnp.float32)
    alibi_bias = slopes[:, None, None] * distance[None]
    causal = positions[None, :] <= positions[:, None]
    diagonal = positions[None, :] == positions[:, None]
    score_scale = HEAD_DIM ** -0.5

    def one_sequence(seq_pair):
        qkv_seq, mask_row = seq_pair
        queries = qkv_seq[:, :, 0].astype(jnp.float32)
        key_vals = qkv_seq[:, :, 1].astype(jnp.float32)
        values = qkv_seq[:, :, 2].astype(jnp.float32)
        scores = jnp.einsum('qhd,khd->hqk', queries, key_vals) * score_scale + alibi_bias
        allowed = (causal & (mask_row[None, :] == 1)) | diagonal
        scores = jnp.where(allowed[None], scores, -1e30)
        attn_probs = jax.nn.softmax(scores, axis=-1).astype(jnp.bfloat16)
        context = jnp.einsum('hqk,khd->qhd', attn_probs.astype(jnp.float32), values)
        return context.astype(jnp.bfloat16).reshape(SEQ, D)

    context = lax.map(one_sequence, (qkv_all, pad_mask)).reshape(BATCH * SEQ, D)
    attn_proj = jnp.dot(context, w_out, preferred_element_type=jnp.float32) + b_out.astype(jnp.float32)
    resid_mid = (resid_in.astype(jnp.float32) + attn_proj).astype(jnp.bfloat16)
    normed2 = layer_norm(resid_mid, ln2_w, ln2_b)
    hidden_up = jnp.dot(normed2, w_up, preferred_element_type=jnp.float32) + b_up.astype(jnp.float32)
    activated = bloom_gelu(hidden_up).astype(jnp.bfloat16)
    down_proj = jnp.dot(activated, w_down, preferred_element_type=jnp.float32) + b_down.astype(jnp.float32)
    result = (resid_mid.astype(jnp.float32) + down_proj).astype(jnp.bfloat16)
    return result.reshape(BATCH, SEQ, D)
```

```python
import functools
import math
import jax
import jax.numpy as jnp
from jax import lax
from jax.experimental import pallas as pl
from jax.experimental.pallas import tpu as pltpu
from jax.sharding import PartitionSpec as P

LN_EPS = 1e-5
BIAS_ROWS = 16


def alibi_slopes(n_heads):
    closest = 2 ** int(math.floor(math.log2(n_heads)))
    base_ratio = 2.0 ** (-(2.0 ** -(math.log2(closest) - 3)))
    extra_ratio = 2.0 ** (-(2.0 ** -(math.log2(2 * closest) - 3)))
    first_part = [base_ratio ** step_k for step_k in range(1, closest + 1)]
    second_part = [extra_ratio ** step_k for step_k in range(1, 2 * (n_heads - closest), 2)]
    return first_part + second_part


def layer_norm(values_in, ln_gain, ln_shift):
    values_in = values_in.astype(jnp.float32)
    mean_v = jnp.mean(values_in, axis=-1, keepdims=True)
    centered = values_in - mean_v
    var_v = jnp.mean(centered * centered, axis=-1, keepdims=True)
    scaled = centered * lax.rsqrt(var_v + LN_EPS)
    return (scaled * ln_gain.astype(jnp.float32) + ln_shift.astype(jnp.float32)).astype(jnp.bfloat16)


def bloom_gelu(values_in):
    return values_in * 0.5 * (1.0 + jnp.tanh(0.79788456 * values_in * (1.0 + 0.044715 * values_in * values_in)))


def attention_kernel(block, slope_ref, pad_ref, q_ref, k_ref, v_ref, out_ref):
    seq_len, head_dim = q_ref.shape
    slope = slope_ref[pl.program_id(0)]
    for first in range(0, seq_len, block):
        n_keys = first + block
        scores = lax.dot_general(q_ref[first:n_keys], k_ref[:n_keys], (((1,), (1,)), ((), ())), preferred_element_type=jnp.float32)
        key_pos = lax.broadcasted_iota(jnp.int32, (block, n_keys), 1)
        query_pos = lax.broadcasted_iota(jnp.int32, (block, n_keys), 0) + first
        distance = key_pos - query_pos
        scores = scores * (head_dim ** -0.5) + slope * distance.astype(jnp.float32)
        allowed = ((distance <= 0) & (pad_ref[:, :n_keys] == 1)) | (distance == 0)
        scores = jnp.where(allowed, scores, -1e30)
        weights = jnp.exp(scores - jnp.max(scores, axis=-1, keepdims=True))
        probs = (weights / jnp.sum(weights, axis=-1, keepdims=True)).astype(jnp.bfloat16)
        out_ref[first:n_keys] = jnp.dot(probs, v_ref[:n_keys], preferred_element_type=jnp.float32).astype(jnp.bfloat16)


def attention(qkv, pad_mask, slopes, heads, head_dim):
    n_seq, seq_len, _ = qkv.shape
    block = math.gcd(seq_len, 256)
    column = lambda part: pl.BlockSpec((None, seq_len, head_dim), lambda h, b: (b, 0, 3 * h + part))
    return pl.pallas_call(
        functools.partial(attention_kernel, block),
        grid=(heads, n_seq),
        in_specs=[pl.BlockSpec(memory_space=pltpu.SMEM), pl.BlockSpec((None, 1, seq_len), lambda h, b: (b, 0, 0)), column(0), column(1), column(2)],
        out_specs=pl.BlockSpec((None, seq_len, head_dim), lambda h, b: (b, 0, h)),
        out_shape=jax.ShapeDtypeStruct((n_seq, seq_len, heads * head_dim), jnp.bfloat16),
        cost_estimate=pl.CostEstimate(flops=4 * n_seq * heads * seq_len * seq_len * head_dim, bytes_accessed=qkv.size * 3, transcendentals=n_seq * heads * seq_len * seq_len // 2),
        name='attention',
    )(slopes, pad_mask[:, None], qkv, qkv, qkv)


def mlp_kernel(row_block, normed_ref, up_ref, down_ref, resid_ref, shift_ref, out_ref, total):
    step = pl.program_id(0)
    rows, width = normed_ref.shape
    up = up_ref[...].reshape(width, up_ref.shape[-1])
    down_rows = down_ref.shape[1] - BIAS_ROWS
    down = down_ref[:, :down_rows].reshape(-1, down_ref.shape[-1])
    bias = down_ref[0, down_rows:, :up.shape[1]][:1].astype(jnp.float32)
    for first in range(0, rows, row_block):
        part = slice(first, first + row_block)
        hidden = jnp.dot(normed_ref[part], up, preferred_element_type=jnp.float32) + bias
        activated = bloom_gelu(hidden).astype(jnp.bfloat16)
        product = jnp.dot(activated, down, preferred_element_type=jnp.float32)

        @pl.when(step == 0)
        def _():
            total[part] = product

        @pl.when(step > 0)
        def _():
            total[part] += product

    @pl.when(step == pl.num_programs(0) - 1)
    def _():
        out_ref[...] = (resid_ref[...].astype(jnp.float32) + total[...] + shift_ref[...].astype(jnp.float32)).astype(jnp.bfloat16)


def mlp(normed, up_all, down_all, resid, shift):
    rows, width = normed.shape
    n_dp, n_tp, up_rows, hidden = up_all.shape
    whole = lambda t: (0, 0)
    return pl.pallas_call(
        functools.partial(mlp_kernel, math.gcd(rows, 256)),
        grid=(n_tp,),
        in_specs=[
            pl.BlockSpec((rows, width), whole),
            pl.BlockSpec((n_dp, None, up_rows, hidden), lambda t: (0, t, 0, 0)),
            pl.BlockSpec((n_dp, None, down_all.shape[2], width), lambda t: (0, t, 0, 0)),
            pl.BlockSpec((rows, width), whole),
            pl.BlockSpec((1, width), whole),
        ],
        out_specs=pl.BlockSpec((rows, width), whole),
        out_shape=jax.ShapeDtypeStruct((rows, width), jnp.bfloat16),
        scratch_shapes=[pltpu.VMEM((rows, width), jnp.float32)],
        compiler_params=pltpu.CompilerParams(vmem_limit_bytes=60 * 1024 * 1024),
        cost_estimate=pl.CostEstimate(flops=4 * rows * width * hidden * n_tp, bytes_accessed=2 * (up_all.size + down_all.size), transcendentals=rows * hidden * n_tp),
        name='mlp',
    )(normed, up_all, down_all, resid, shift)


def solution(mesh):
    n_tp, n_dp = mesh.shape['tp'], mesh.shape['dp']

    def gather_weight(shard, extra=None):
        rows = shard.shape[0] // n_dp
        part = lax.dynamic_slice_in_dim(shard, lax.axis_index('dp') * rows, rows)
        if extra is not None:
            part = jnp.concatenate([part, jnp.pad(extra[None], ((0, BIAS_ROWS - 1), (0, shard.shape[1] - extra.shape[0])))])
        return lax.all_gather(part, ('dp', 'tp'), axis=0, tiled=True).reshape(n_dp, n_tp, part.shape[0], shard.shape[1])

    def local_step(tok_ids, pad_mask, emb_shard, ln_emb_w, ln_emb_b, ln1_w, ln1_b, w_qkv, b_qkv, w_out, b_out, ln2_w, ln2_b, w_up, b_up, w_down, b_down):
        tp_rank = lax.axis_index('tp')
        vocab_loc, width = emb_shard.shape
        heads_loc, head_dim = w_qkv.shape[1], w_qkv.shape[3]
        n_seq, seq_len = tok_ids.shape
        seq_loc = seq_len // n_tp
        up_all, down_all, out_all = gather_weight(w_up), gather_weight(w_down, b_up), gather_weight(w_out)
        all_slopes = jnp.array(alibi_slopes(heads_loc * n_tp), jnp.float32)
        head_slopes = lax.dynamic_slice_in_dim(all_slopes, tp_rank * heads_loc, heads_loc)
        local_ids = tok_ids - tp_rank * vocab_loc
        in_range = (local_ids >= 0) & (local_ids < vocab_loc)
        looked_up = jnp.take(emb_shard, jnp.clip(local_ids, 0, vocab_loc - 1), axis=0)
        partial_emb = jnp.where(in_range[:, :, None], looked_up, jnp.zeros((), jnp.bfloat16))
        partial_emb, up_all, down_all, out_all = lax.optimization_barrier((partial_emb, up_all, down_all, out_all))
        out_all = out_all.transpose(1, 0, 2, 3).reshape(-1, width)
        embedded = lax.psum_scatter(partial_emb, 'tp', scatter_dimension=1, tiled=True)
        resid_in = layer_norm(embedded, ln_emb_w, ln_emb_b)
        normed = layer_norm(resid_in, ln1_w, ln1_b)
        normed_all = lax.all_gather(normed, 'tp', axis=1, tiled=True)
        qkv = (jnp.einsum('bsd,de->bse', normed_all, w_qkv.reshape(width, -1), preferred_element_type=jnp.float32) + b_qkv.reshape(-1).astype(jnp.float32)).astype(jnp.bfloat16)
        context = attention(qkv, pad_mask, head_slopes, heads_loc, head_dim)
        context = lax.all_to_all(context.reshape(n_seq, n_tp, seq_loc, heads_loc * head_dim), 'tp', 1, 3, tiled=True).reshape(n_seq * seq_loc, width)
        attn_proj = jnp.dot(context, out_all, preferred_element_type=jnp.float32)
        resid_mid = (resid_in.reshape(-1, width).astype(jnp.float32) + attn_proj + b_out.astype(jnp.float32)).astype(jnp.bfloat16)
        normed2 = layer_norm(resid_mid, ln2_w, ln2_b)
        out = mlp(normed2, up_all, down_all, resid_mid, b_down[None])
        return out.reshape(n_seq, seq_loc, width)

    replicated = P(None)
    in_specs = (P('dp', None), P('dp', None), P('tp', None), replicated, replicated, replicated, replicated, P(None, 'tp', None, None), P('tp', None, None), P('tp', None), replicated, replicated, replicated, P(None, 'tp'), P('tp'), P('tp', None), replicated)
    return jax.shard_map(local_step, mesh=mesh, in_specs=in_specs, out_specs=P('dp', 'tp', None), check_vma=False)
```

```python
import functools
import math
import jax
import jax.numpy as jnp
from jax import lax
from jax.experimental import pallas as pl
from jax.experimental.pallas import tpu as pltpu
from jax.sharding import PartitionSpec as P

LN_EPS = 1e-5
BIAS_ROWS = 16


def alibi_slopes(n_heads):
    closest = 2 ** int(math.floor(math.log2(n_heads)))
    base_ratio = 2.0 ** (-(2.0 ** -(math.log2(closest) - 3)))
    extra_ratio = 2.0 ** (-(2.0 ** -(math.log2(2 * closest) - 3)))
    first_part = [base_ratio ** step_k for step_k in range(1, closest + 1)]
    second_part = [extra_ratio ** step_k for step_k in range(1, 2 * (n_heads - closest), 2)]
    return first_part + second_part


def layer_norm(values_in, ln_gain, ln_shift):
    values_in = values_in.astype(jnp.float32)
    mean_v = jnp.mean(values_in, axis=-1, keepdims=True)
    centered = values_in - mean_v
    var_v = jnp.mean(centered * centered, axis=-1, keepdims=True)
    scaled = centered * lax.rsqrt(var_v + LN_EPS)
    return (scaled * ln_gain.astype(jnp.float32) + ln_shift.astype(jnp.float32)).astype(jnp.bfloat16)


def bloom_gelu(values_in):
    return values_in * 0.5 * (1.0 + jnp.tanh(0.79788456 * values_in * (1.0 + 0.044715 * values_in * values_in)))


def attention_kernel(block, slope_ref, pad_ref, q_ref, k_ref, v_ref, out_ref):
    seq_len, head_dim = q_ref.shape
    slope = slope_ref[pl.program_id(0)]
    for first in range(0, seq_len, block):
        n_keys = first + block
        scores = lax.dot_general(q_ref[first:n_keys], k_ref[:n_keys], (((1,), (1,)), ((), ())), preferred_element_type=jnp.float32)
        key_pos = lax.broadcasted_iota(jnp.int32, (block, n_keys), 1)
        query_pos = lax.broadcasted_iota(jnp.int32, (block, n_keys), 0) + first
        distance = key_pos - query_pos
        scores = scores * (head_dim ** -0.5) + slope * distance.astype(jnp.float32)
        allowed = ((distance <= 0) & (pad_ref[:, :n_keys] == 1)) | (distance == 0)
        scores = jnp.where(allowed, scores, -1e30)
        weights = jnp.exp(scores - jnp.max(scores, axis=-1, keepdims=True))
        probs = (weights / jnp.sum(weights, axis=-1, keepdims=True)).astype(jnp.bfloat16)
        out_ref[first:n_keys] = jnp.dot(probs, v_ref[:n_keys], preferred_element_type=jnp.float32).astype(jnp.bfloat16)


def attention(qkv, pad_mask, slopes, heads, head_dim):
    n_seq, seq_len, _ = qkv.shape
    block = math.gcd(seq_len, 256)
    column = lambda part: pl.BlockSpec((None, seq_len, head_dim), lambda h, b: (b, 0, 3 * h + part))
    return pl.pallas_call(
        functools.partial(attention_kernel, block),
        grid=(heads, n_seq),
        in_specs=[pl.BlockSpec(memory_space=pltpu.SMEM), pl.BlockSpec((None, 1, seq_len), lambda h, b: (b, 0, 0)), column(0), column(1), column(2)],
        out_specs=pl.BlockSpec((None, seq_len, head_dim), lambda h, b: (b, 0, h)),
        out_shape=jax.ShapeDtypeStruct((n_seq, seq_len, heads * head_dim), jnp.bfloat16),
        cost_estimate=pl.CostEstimate(flops=4 * n_seq * heads * seq_len * seq_len * head_dim, bytes_accessed=qkv.size * 3, transcendentals=n_seq * heads * seq_len * seq_len // 2),
        name='attention',
    )(slopes, pad_mask[:, None], qkv, qkv, qkv)


def up_kernel(row_block, normed_ref, up_ref, out_ref):
    rows, width = normed_ref.shape
    up_rows = up_ref.shape[1] - BIAS_ROWS
    up = up_ref[:, :up_rows].reshape(width, up_ref.shape[-1])
    bias = up_ref[0, up_rows:][:1].astype(jnp.float32)
    for first in range(0, rows, row_block):
        part = slice(first, first + row_block)
        hidden = jnp.dot(normed_ref[part], up, preferred_element_type=jnp.float32) + bias
        out_ref[part] = bloom_gelu(hidden).astype(jnp.bfloat16)


def mlp_up(normed, up_all):
    rows, width = normed.shape
    n_dp, n_tp, up_rows, hidden = up_all.shape
    return pl.pallas_call(
        functools.partial(up_kernel, math.gcd(rows, 256)),
        grid=(n_tp,),
        in_specs=[pl.BlockSpec((rows, width), lambda t: (0, 0)), pl.BlockSpec((n_dp, None, up_rows, hidden), lambda t: (0, t, 0, 0))],
        out_specs=pl.BlockSpec((rows, hidden), lambda t: (0, t)),
        out_shape=jax.ShapeDtypeStruct((rows, hidden * n_tp), jnp.bfloat16),
        compiler_params=pltpu.CompilerParams(vmem_limit_bytes=56 * 1024 * 1024),
        cost_estimate=pl.CostEstimate(flops=2 * rows * width * hidden * n_tp, bytes_accessed=2 * up_all.size, transcendentals=rows * hidden * n_tp),
        name='mlp_up',
    )(normed, up_all)


def down_kernel(row_block, act_ref, down_ref, resid_ref, shift_ref, out_ref, total):
    step = pl.program_id(0)
    down = down_ref[...].reshape(-1, down_ref.shape[-1])
    for first in range(0, act_ref.shape[0], row_block):
        part = slice(first, first + row_block)
        product = jnp.dot(act_ref[part], down, preferred_element_type=jnp.float32)

        @pl.when(step == 0)
        def _():
            total[part] = product

        @pl.when(step > 0)
        def _():
            total[part] += product

    @pl.when(step == pl.num_programs(0) - 1)
    def _():
        out_ref[...] = (resid_ref[...].astype(jnp.float32) + total[...] + shift_ref[...].astype(jnp.float32)).astype(jnp.bfloat16)


def mlp_down(activated, down_all, resid, shift):
    rows, width = resid.shape
    n_dp, n_tp, down_rows, _ = down_all.shape
    whole = lambda t: (0, 0)
    return pl.pallas_call(
        functools.partial(down_kernel, math.gcd(rows, 256)),
        grid=(n_tp,),
        in_specs=[
            pl.BlockSpec((rows, n_dp * down_rows), lambda t: (0, t)),
            pl.BlockSpec((n_dp, None, down_rows, width), lambda t: (0, t, 0, 0)),
            pl.BlockSpec((rows, width), whole),
            pl.BlockSpec((1, width), whole),
        ],
        out_specs=pl.BlockSpec((rows, width), whole),
        out_shape=jax.ShapeDtypeStruct((rows, width), jnp.bfloat16),
        scratch_shapes=[pltpu.VMEM((rows, width), jnp.float32)],
        compiler_params=pltpu.CompilerParams(vmem_limit_bytes=56 * 1024 * 1024),
        cost_estimate=pl.CostEstimate(flops=2 * rows * width * n_dp * down_rows * n_tp, bytes_accessed=2 * down_all.size, transcendentals=0),
        name='mlp_down',
    )(activated, down_all, resid, shift)


def solution(mesh):
    n_tp, n_dp = mesh.shape['tp'], mesh.shape['dp']

    def gather_weight(shard, extra=None):
        rows = shard.shape[0] // n_dp
        part = lax.dynamic_slice_in_dim(shard, lax.axis_index('dp') * rows, rows)
        if extra is not None:
            part = jnp.concatenate([part, jnp.pad(extra[None], ((0, BIAS_ROWS - 1), (0, shard.shape[1] - extra.shape[0])))])
        return lax.all_gather(part, ('dp', 'tp'), axis=0, tiled=True).reshape(n_dp, n_tp, part.shape[0], shard.shape[1])

    def local_step(tok_ids, pad_mask, emb_shard, ln_emb_w, ln_emb_b, ln1_w, ln1_b, w_qkv, b_qkv, w_out, b_out, ln2_w, ln2_b, w_up, b_up, w_down, b_down):
        tp_rank = lax.axis_index('tp')
        vocab_loc, width = emb_shard.shape
        heads_loc, head_dim = w_qkv.shape[1], w_qkv.shape[3]
        n_seq, seq_len = tok_ids.shape
        seq_loc = seq_len // n_tp
        up_all, out_all = gather_weight(w_up, b_up), gather_weight(w_out)
        all_slopes = jnp.array(alibi_slopes(heads_loc * n_tp), jnp.float32)
        head_slopes = lax.dynamic_slice_in_dim(all_slopes, tp_rank * heads_loc, heads_loc)
        local_ids = tok_ids - tp_rank * vocab_loc
        in_range = (local_ids >= 0) & (local_ids < vocab_loc)
        looked_up = jnp.take(emb_shard, jnp.clip(local_ids, 0, vocab_loc - 1), axis=0)
        partial_emb = jnp.where(in_range[:, :, None], looked_up, jnp.zeros((), jnp.bfloat16))
        partial_emb, up_all, out_all = lax.optimization_barrier((partial_emb, up_all, out_all))
        out_all = out_all.transpose(1, 0, 2, 3).reshape(-1, width)
        embedded = lax.psum_scatter(partial_emb, 'tp', scatter_dimension=1, tiled=True)
        resid_in = layer_norm(embedded, ln_emb_w, ln_emb_b)
        normed = layer_norm(resid_in, ln1_w, ln1_b)
        normed_all, down_shard = lax.optimization_barrier((lax.all_gather(normed, 'tp', axis=1, tiled=True), w_down))
        down_all = gather_weight(down_shard)
        qkv = (jnp.einsum('bsd,de->bse', normed_all, w_qkv.reshape(width, -1), preferred_element_type=jnp.float32) + b_qkv.reshape(-1).astype(jnp.float32)).astype(jnp.bfloat16)
        context = attention(qkv, pad_mask, head_slopes, heads_loc, head_dim)
        context = lax.all_to_all(context.reshape(n_seq, n_tp, seq_loc, heads_loc * head_dim), 'tp', 1, 3, tiled=True).reshape(n_seq * seq_loc, width)
        attn_proj = jnp.dot(context, out_all, preferred_element_type=jnp.float32)
        resid_mid = (resid_in.reshape(-1, width).astype(jnp.float32) + attn_proj + b_out.astype(jnp.float32)).astype(jnp.bfloat16)
        normed2 = layer_norm(resid_mid, ln2_w, ln2_b)
        out = mlp_down(mlp_up(normed2, up_all), down_all, resid_mid, b_down[None])
        return out.reshape(n_seq, seq_loc, width)

    replicated = P(None)
    in_specs = (P('dp', None), P('dp', None), P('tp', None), replicated, replicated, replicated, replicated, P(None, 'tp', None, None), P('tp', None, None), P('tp', None), replicated, replicated, replicated, P(None, 'tp'), P('tp'), P('tp', None), replicated)
    return jax.shard_map(local_step, mesh=mesh, in_specs=in_specs, out_specs=P('dp', 'tp', None), check_vma=False)
```
